16 devices in a mesh: rep: 2 (over y, z), dp: 8 (over x, core).
Axes of the slice: x: 4, y: 2, z: 1, core: 2. Of those that a mesh axis runs over, the one named last changes fastest.
The devices are a block of a 4x4x8 slice.
Arguments:
- g_w_gate: bfloat16 [16, 2, 1152, 4608], P(('rep', 'dp')), parts along dimension 0
- g_w_up: bfloat16 [16, 2, 1152, 4608], P(('rep', 'dp')), parts along dimension 0
- g_w_down: bfloat16 [16, 2, 4608, 1152], P(('rep', 'dp')), parts along dimension 0
- w_gate: bfloat16 [2, 1152, 4608], replicated
- w_up: bfloat16 [2, 1152, 4608], replicated
- w_down: bfloat16 [2, 4608, 1152], replicated
- m_w_gate: float32 [2, 1152, 4608], P(None, 'dp')
- m_w_up: float32 [2, 1152, 4608], P(None, 'dp')
- m_w_down: float32 [2, 4608, 1152], P(None, 'dp')
- v_w_gate: float32 [2, 1152, 4608], P(None, 'dp')
- v_w_up: float32 [2, 1152, 4608], P(None, 'dp')
- v_w_down: float32 [2, 4608, 1152], P(None, 'dp')
Outputs:
- output 1: bfloat16 [4, 1152, 4608], P('rep'), parts along dimension 0
- output 2: bfloat16 [4, 1152, 4608], P('rep'), parts along dimension 0
- output 3: bfloat16 [4, 4608, 1152], P('rep'), parts along dimension 0
- output 4: float32 [4, 1152, 4608], P('rep', 'dp'), parts along dimension 0
- output 5: float32 [4, 1152, 4608], P('rep', 'dp'), parts along dimension 0
- output 6: float32 [4, 4608, 1152], P('rep', 'dp'), parts along dimension 0
- output 7: float32 [4, 1152, 4608], P('rep', 'dp'), parts along dimension 0
- output 8: float32 [4, 1152, 4608], P('rep', 'dp'), parts along dimension 0
- output 9: float32 [4, 4608, 1152], P('rep', 'dp'), parts along dimension 0
There are 2 independent parts. The reference program is written for one: setup_inputs(seed, part) draws one part's arguments, and reference() takes and returns one part's arrays. A program takes and returns all parts, laid end to end along the dimension named above; an argument that names none is the same for every part.
All inputs are finite; a program needn't handle non-finite values.
Results may differ from the reference program's by a relative error of at most 0.022.
Values are sent between devices in bfloat16 or wider.
A program may use at most 768 MiB of HBM per device.

```python
import jax
import jax.numpy as jnp
from jax import lax

DEVICES = 8
D = 1152
FF = 4608
LAYERS = 2
NAMES = ("w_gate", "w_up", "w_down")
SHAPES = {"w_gate": (LAYERS, D, FF), "w_up": (LAYERS, D, FF), "w_down": (LAYERS, FF, D)}


def setup_inputs(seed: int = 0, part: int = 0) -> dict:
    kz, *keys = jax.random.split(jax.random.key(seed), 1 + 5 * len(NAMES))
    loud = 2.0 ** jax.random.uniform(kz, (), jnp.float32, -1.0, 1.0)
    drawn = {}
    for name, key, both in zip(NAMES, keys[:3], keys[3:6], strict=True):
        own = jax.random.normal(jax.random.fold_in(key, part), (DEVICES, *SHAPES[name]), jnp.float32)
        shared = jax.random.normal(jax.random.fold_in(both, part), SHAPES[name], jnp.float32)
        drawn["g_" + name] = (loud * (0.7 * shared / DEVICES + 0.7 * own * DEVICES**-0.5)).astype(jnp.bfloat16)
    for name, key in zip(NAMES, keys[6:9], strict=True):
        drawn[name] = (jax.random.normal(key, SHAPES[name], jnp.float32) * SHAPES[name][1] ** -0.5).astype(jnp.bfloat16)
    for name, key in zip(NAMES, keys[9:12], strict=True):
        drawn["m_" + name] = loud * 0.5 * jax.random.normal(key, SHAPES[name], jnp.float32)
    for name, key in zip(NAMES, keys[12:15], strict=True):
        drawn["v_" + name] = loud * loud * jax.random.uniform(key, SHAPES[name], jnp.float32, 0.5, 1.5)
    return drawn


def adamw(w, m, v, g):
    m = 0.9 * m + 0.1 * g
    v = 0.95 * v + 0.05 * g * g
    step = m * lax.rsqrt(v + 1e-8) + 0.1 * w
    return (w - 0.02 * step).astype(jnp.bfloat16), m, v


def reference(g_w_gate, g_w_up, g_w_down, w_gate, w_up, w_down, m_w_gate, m_w_up, m_w_down, v_w_gate, v_w_up, v_w_down):
    def total(terms):
        return lax.scan(lambda so_far, term: (so_far + term.astype(jnp.float32), None), jnp.zeros(terms.shape[1:], jnp.float32), terms)[0]

    gradients = [total(terms).astype(jnp.bfloat16).astype(jnp.float32) for terms in (g_w_gate, g_w_up, g_w_down)]
    new = [
        adamw(w.astype(jnp.float32), m, v, g)
        for w, m, v, g in zip((w_gate, w_up, w_down), (m_w_gate, m_w_up, m_w_down), (v_w_gate, v_w_up, v_w_down), gradients, strict=True)
    ]
    return tuple(one[which] for which in range(3) for one in new)
```

```python
import functools

import jax
import jax.numpy as jnp
from jax import lax
from jax.experimental import pallas as pl
from jax.experimental.pallas import tpu as pltpu
from jax.sharding import PartitionSpec as P

CORES = 2
PIECES = 4
STRIP = 16
MESH = pl.DeviceIdType.MESH
ORDER = (2, 1, 3, 0)


def reduce_kernel(chips, layers, *refs):
    weights = 3
    terms, old, ms, vs = (refs[i : i + weights] for i in range(0, 4 * weights, weights))
    units = weights * layers
    fresh = refs[4 * weights : 4 * weights + units]
    grads = refs[4 * weights + units : 5 * weights + units]
    (own, oth, m_in, v_in, w_in, w_out, g_out, far, near, from_far, from_near,
     own_sem, oth_send, oth_recv, old_sem, out_sem, far_send, far_recv, near_send, near_recv, free_sem) = refs[5 * weights + units :]
    rows, columns = own.shape[-2:]
    chunks = units * 2
    me = lax.axis_index("dp")
    x, k = me // CORES, lax.rem(me, CORES)
    right = {"dp": lax.rem(x + 1, chips) * CORES + k}
    left = {"dp": lax.rem(x + chips - 1, chips) * CORES + k}
    partner = {"dp": x * CORES + 1 - k}

    barrier = pltpu.get_barrier_semaphore()
    for who in (right, left, partner):
        pl.semaphore_signal(barrier, inc=1, device_id=who, device_id_type=MESH)
    pl.semaphore_wait(barrier, 3)

    def piece(ref, lead, block, p):
        if ref.shape[-1] == columns:
            return ref.at[(*lead, pl.ds(pl.multiple_of((block * PIECES + p) * rows, 8), rows))]
        return ref.at[(*lead, pl.ds(pl.multiple_of(block * rows, 8), rows), pl.ds(pl.multiple_of(p * columns, 128), columns))]

    def for_weight(c, body):
        for i in range(weights):
            pl.when(c // (layers * 2) == i)(functools.partial(body, i, lax.rem(c // 2, layers), lax.rem(c, 2)))

    def load(c):
        slot = lax.rem(c, 4)

        def start(i, layer, h):
            for group in ((0,), (1, 2, 3)):
                late = min(group[0], 1)
                for j in group:
                    block = lax.rem(x + ORDER[j], chips) * CORES
                    for q in range(2):
                        pltpu.make_async_remote_copy(
                            src_ref=piece(terms[i], (0, layer), block + 1 - k, h * 2 + q),
                            dst_ref=oth.at[slot, j, q],
                            send_sem=oth_send.at[slot, late],
                            recv_sem=oth_recv.at[slot, late],
                            device_id=partner,
                            device_id_type=MESH,
                        ).start()
                        pltpu.make_async_copy(piece(terms[i], (0, layer), block + k, h * 2 + q), own.at[slot, j, q], own_sem.at[slot, late]).start()

        for_weight(c, start)

    def load_old(c):
        slot = lax.rem(c, 2)

        def start(i, layer, h):
            for q in range(2):
                p = h * 2 + q
                pltpu.make_async_copy(piece(ms[i], (layer,), 0, p), m_in.at[slot, q], old_sem.at[slot, 0]).start()
                pltpu.make_async_copy(piece(vs[i], (layer,), 0, p), v_in.at[slot, q], old_sem.at[slot, 1]).start()
                pltpu.make_async_copy(piece(old[i], (layer,), me, p), w_in.at[slot, q], old_sem.at[slot, 2]).start()

        for_weight(c, start)

    def wait_for(ref, sem):
        pltpu.make_async_copy(ref, ref, sem).wait()

    def wait_terms(slot, late):
        part = pl.ds(late, 3) if late else pl.ds(0, 1)
        wait_for(own.at[slot, part], own_sem.at[slot, late])
        wait_for(oth.at[slot, part], oth_recv.at[slot, late])
        wait_for(oth.at[slot, part], oth_send.at[slot, late])

    def strips(body):
        @pl.loop(0, rows // STRIP)
        def _(r):
            body(pl.ds(pl.multiple_of(r * STRIP, STRIP), STRIP))

    def pair(slot, j, q, at):
        return own[slot, j, q, at].astype(jnp.float32) + oth[slot, j, q, at].astype(jnp.float32)

    def far_copy(c, q):
        return pltpu.make_async_remote_copy(
            src_ref=far.at[lax.rem(c, 2), q],
            dst_ref=from_far.at[c, q],
            send_sem=far_send.at[lax.rem(c, 2), q],
            recv_sem=far_recv.at[c, q],
            device_id=(right, left)[q],
            device_id_type=MESH,
        )

    def near_copy(c, d):
        return pltpu.make_async_remote_copy(
            src_ref=near.at[lax.rem(c, 2), d],
            dst_ref=from_near.at[c, d],
            send_sem=near_send.at[lax.rem(c, 2), d],
            recv_sem=near_recv.at[c, d],
            device_id=(right, left)[d],
            device_id_type=MESH,
        )

    def send_far(c):
        slot = lax.rem(c, 4)
        wait_terms(slot, 0)

        @pl.when(c >= 2)
        def _():
            for q in range(2):
                far_copy(c - 2, q).wait_send()

        def strip(at):
            for q in range(2):
                far[lax.rem(c, 2), q, at] = pair(slot, 0, q, at).astype(far.dtype)

        strips(strip)
        for q in range(2):
            far_copy(c, q).start()

    def send_near(c):
        slot = lax.rem(c, 4)
        wait_terms(slot, 1)

        @pl.when(c >= 2)
        def _():
            for d in range(2):
                near_copy(c - 2, d).wait_send()

        for q in range(2):
            far_copy(c, q).wait_recv()

        def strip(at):
            for d in range(2):
                for q in range(2):
                    total = pair(slot, 1 + d, q, at)
                    if q == d:
                        total += from_far[c, q, at].astype(jnp.float32)
                    near[lax.rem(c, 2), d, q, at] = total.astype(near.dtype)

        strips(strip)
        for d in range(2):
            near_copy(c, d).start()

    def outputs(c, act):
        slot = lax.rem(c, 2)

        def go(i, layer, h):
            for q in range(2):
                p = h * 2 + q
                act(pltpu.make_async_copy(g_out.at[slot, q], piece(grads[i], (layer,), 0, p), out_sem.at[slot, q, 0]))
                for which in range(layers):

                    @pl.when(layer == which)
                    def _():
                        act(pltpu.make_async_copy(w_out.at[slot, q], piece(fresh[i * layers + which], (), 0, p), out_sem.at[slot, q, 1]))

        for_weight(c, go)

    def finish(c):
        slot, two = lax.rem(c, 4), lax.rem(c, 2)
        wait_for(m_in.at[two], old_sem.at[two, 0])
        wait_for(v_in.at[two], old_sem.at[two, 1])
        wait_for(w_in.at[two], old_sem.at[two, 2])

        @pl.when(c >= 2)
        def _():
            outputs(c - 2, lambda copy: copy.wait())

        for d in range(2):
            near_copy(c, d).wait_recv()

        def strip(at):
            for q in range(2):
                total = pair(slot, 3, q, at) + from_near[c, 0, q, at].astype(jnp.float32) + from_near[c, 1, q, at].astype(jnp.float32)
                g = total.astype(g_out.dtype)
                g_out[two, q, at] = g
                g = g.astype(jnp.float32)
                w = w_in[two, q, at].astype(jnp.float32)
                m = 0.9 * m_in[two, q, at] + 0.1 * g
                v = 0.95 * v_in[two, q, at] + 0.05 * g * g
                w_out[two, q, at] = (w - 0.02 * (m * lax.rsqrt(v + 1e-8) + 0.1 * w)).astype(w_out.dtype)

        strips(strip)
        outputs(c, lambda copy: copy.start())

        @pl.when(c + 4 < chunks)
        def _():
            pl.semaphore_signal(free_sem, inc=1, device_id=partner, device_id_type=MESH)

    @pl.loop(0, chunks + 3)
    def _(s):
        @pl.when(s < chunks)
        def _():
            @pl.when(s >= 4)
            def _():
                pl.semaphore_wait(free_sem, 1)

            load(s)

        @pl.when((s >= 1) & (s < chunks + 1))
        def _():
            send_far(s - 1)

        @pl.when((s >= 2) & (s < chunks + 2))
        def _():
            load_old(s - 2)
            send_near(s - 2)

        @pl.when(s >= 3)
        def _():
            finish(s - 3)

    for c in (chunks - 2, chunks - 1):
        for q in range(2):
            far_copy(c, q).wait_send()
            near_copy(c, q).wait_send()
        outputs(c, lambda copy: copy.wait())


def reduce_and_step(chips, terms, weights, ms, vs):
    layers = terms[0].shape[1]
    units = [(i, layer) for i in range(3) for layer in range(layers)]
    chunks = len(units) * 2
    rows, columns = min(m.shape[1] for m in ms), min(m.shape[2] for m in ms)
    bf, f32 = jnp.bfloat16, jnp.float32
    tile = (rows, columns)
    dma = pltpu.SemaphoreType.DMA
    out = pl.pallas_call(
        functools.partial(reduce_kernel, chips, layers),
        out_shape=[jax.ShapeDtypeStruct(ms[i].shape[1:], bf) for i, _ in units] + [jax.ShapeDtypeStruct(m.shape, bf) for m in ms],
        in_specs=[pl.BlockSpec(memory_space=pl.ANY)] * 12,
        out_specs=[pl.BlockSpec(memory_space=pl.ANY)] * (len(units) + 3),
        scratch_shapes=[
            pltpu.VMEM((4, 4, 2, *tile), bf),
            pltpu.VMEM((4, 4, 2, *tile), bf),
            pltpu.VMEM((2, 2, *tile), f32),
            pltpu.VMEM((2, 2, *tile), f32),
            pltpu.VMEM((2, 2, *tile), bf),
            pltpu.VMEM((2, 2, *tile), bf),
            pltpu.VMEM((2, 2, *tile), bf),
            pltpu.VMEM((2, 2, *tile), bf),
            pltpu.VMEM((2, 2, 2, *tile), bf),
            pltpu.VMEM((chunks, 2, *tile), bf),
            pltpu.VMEM((chunks, 2, 2, *tile), bf),
            dma((4, 2)),
            dma((4, 2)),
            dma((4, 2)),
            dma((2, 3)),
            dma((2, 2, 2)),
            dma((2, 2)),
            dma((chunks, 2)),
            dma((2, 2)),
            dma((chunks, 2)),
            pltpu.SemaphoreType.REGULAR,
        ],
        compiler_params=pltpu.CompilerParams(collective_id=0, has_side_effects=True, vmem_limit_bytes=67_000_000),
        name="reduce",
    )(*terms, *weights, *ms, *vs)
    return dict(zip(units, out)), out[len(units) :]


def place_kernel(layer, chips, jobs, count, *refs):
    out, buf, in_sem, out_sem = refs[-4:]
    me = lax.axis_index("dp")
    x, k = me // CORES, lax.rem(me, CORES)
    copies = []
    for i, (rows, step, at, block_rows, other) in enumerate(jobs):
        block = lax.rem(x + step, chips) * CORES + (1 - k if other else k)
        slot = buf.at[i, pl.ds(0, rows)]
        into = out.at[layer, pl.ds(pl.multiple_of(block * block_rows + at, 8), rows)]
        copies.append((pltpu.make_async_copy(refs[i], slot, in_sem.at[i]), pltpu.make_async_copy(slot, into, out_sem.at[i])))
        copies[i][0].start()
    for first, second in copies:
        first.wait()
        second.start()
    for _, second in copies:
        second.wait()


def place(layer, chips, shape, pieces, so_far):
    arrays = [p[0] for p in pieces]
    jobs = [(p[0].shape[0], *p[1:]) for p in pieces]
    rows, columns = max(j[0] for j in jobs), arrays[0].shape[1]
    extra = () if so_far is None else (so_far,)
    return pl.pallas_call(
        functools.partial(place_kernel, layer, chips, jobs, len(jobs)),
        out_shape=jax.ShapeDtypeStruct(shape, jnp.bfloat16),
        in_specs=[pl.BlockSpec(memory_space=pl.ANY)] * (len(jobs) + len(extra)),
        out_specs=pl.BlockSpec(memory_space=pl.ANY),
        scratch_shapes=[
            pltpu.VMEM((len(jobs), rows, columns), jnp.bfloat16),
            pltpu.SemaphoreType.DMA((len(jobs),)),
            pltpu.SemaphoreType.DMA((len(jobs),)),
        ],
        input_output_aliases={len(jobs): 0} if extra else {},
        cost_estimate=pl.CostEstimate(flops=20_000_000, bytes_accessed=4 * sum(a.size for a in arrays), transcendentals=0),
        name="place",
    )(*arrays, *extra)


def solution(mesh):
    n = mesh.shape["dp"]
    chips = n // CORES

    def pairs(step, flip=0):
        return [(x * CORES + k, (x + step) % chips * CORES + (k + flip) % CORES) for x in range(chips) for k in range(CORES)]

    right, left, partner = pairs(1), pairs(-1), pairs(0, 1)

    def send(a, where):
        return lax.ppermute(a, "dp", where)

    def step(*arrays):
        terms, weights, ms, vs = (arrays[i : i + 3] for i in (0, 3, 6, 9))
        layers = terms[0].shape[1]
        f32 = jnp.float32
        fresh, gradients = reduce_and_step(chips, terms, weights, ms, vs)

        def after(value, *earlier):
            return lax.optimization_barrier((value, *earlier))

        units = list(fresh)
        whole, new_m, new_v = [None] * 3, [None] * 3, [None] * 3
        got = {}

        def send_near(at):
            u = units[at]
            s = fresh[u]
            if at >= 2:
                before = units[at - 2]
                s, *got[before] = after(s, *got[before])
            got[u] = [send(s, right), send(s, left)]

        def put(u, pieces):
            i, layer = u
            rows = fresh[u].shape[0]
            both = [(a, *where, rows, False) for a, *where in pieces] + [(send(a, partner), *where, rows, True) for a, *where in pieces]
            whole[i] = place(layer, chips, weights[i].shape, both, whole[i])

        for at in range(min(2, len(units))):
            send_near(at)
        for at, u in enumerate(units):
            s, half = fresh[u], fresh[u].shape[0] // 2
            a, b = got[u]
            first, second = a[:half], b[half:]
            if at >= 2:
                j = units[at - 2][0]
                first, second, whole[j] = after(first, second, whole[j])
            if 1 <= at <= 3:
                w = at - 1
                g = gradients[w].astype(f32)
                new_m[w] = 0.9 * ms[w] + 0.1 * g
                new_v[w] = 0.95 * vs[w] + 0.05 * g * g
                first, new_m[w], new_v[w] = after(first, new_m[w], new_v[w])
            c, d = send(first, right), send(second, left)
            if at + 2 < len(units):
                send_near(at + 2)
            a, b = got[u]
            put(u, [(s, 0, 0), (a, chips - 1, 0), (b, 1, 0)])
            c, d, whole[u[0]] = after(c, d, whole[u[0]])
            put(u, [(c, 2, 0), (d, 2, half)])
        return (*whole, *new_m, *new_v)

    all_of, cut = P(None, None, None), P(None, "dp", None)
    return jax.shard_map(
        step,
        mesh=mesh,
        in_specs=(P(("rep", "dp"), None, None, None),) * 3 + (all_of,) * 3 + (cut,) * 6,
        out_specs=(P("rep", None, None),) * 3 + (P("rep", "dp", None),) * 6,
        check_vma=False,
    )
```

```python
import functools

import jax
import jax.numpy as jnp
from jax import lax
from jax.experimental import pallas as pl
from jax.experimental.pallas import tpu as pltpu
from jax.sharding import PartitionSpec as P


CORES = 2
PIECES = 4
STRIP = 16
MESH = pl.DeviceIdType.MESH
ORDER = (2, 1, 3, 0)


def reduce_kernel(chips, layers, parts, *refs):
    weights = 3
    terms, old, ms, vs = (refs[i : i + weights] for i in range(0, 4 * weights, weights))
    units = weights * layers
    count = len(parts)
    outs = refs[4 * weights : 5 * weights + 2 * count + 2]
    fresh, other, grads = outs[:count], outs[count : 2 * count], outs[2 * count : 2 * count + weights]
    first = outs[-2:]
    (own, oth, m_in, v_in, w_in, w_out, g_out, far, near, from_far, from_near,
     own_sem, oth_send, oth_recv, old_sem, out_sem, far_send, far_recv, near_send, near_recv,
     other_send, other_recv, first_send, first_recv, free_sem) = refs[5 * weights + 2 * count + 2 :]
    rows, columns = own.shape[-2:]
    chunks = units * 2
    me = lax.axis_index("dp")
    x, k = me // CORES, lax.rem(me, CORES)
    right = {"dp": lax.rem(x + 1, chips) * CORES + k}
    left = {"dp": lax.rem(x + chips - 1, chips) * CORES + k}
    partner = {"dp": x * CORES + 1 - k}

    barrier = pltpu.get_barrier_semaphore()
    for who in (right, left, partner):
        pl.semaphore_signal(barrier, inc=1, device_id=who, device_id_type=MESH)
    pl.semaphore_wait(barrier, 3)

    def piece(ref, lead, block, p):
        if ref.shape[-1] == columns:
            return ref.at[(*lead, pl.ds(pl.multiple_of((block * PIECES + p) * rows, 8), rows))]
        return ref.at[(*lead, pl.ds(pl.multiple_of(block * rows, 8), rows), pl.ds(pl.multiple_of(p * columns, 128), columns))]

    def for_weight(c, body):
        for i in range(weights):
            pl.when(c // (layers * 2) == i)(functools.partial(body, i, lax.rem(c // 2, layers), lax.rem(c, 2)))

    def load(c):
        slot = lax.rem(c, 4)

        def start(i, layer, h):
            for group in ((0,), (1, 2, 3)):
                late = min(group[0], 1)
                for j in group:
                    block = lax.rem(x + ORDER[j], chips) * CORES
                    for q in range(2):
                        pltpu.make_async_remote_copy(
                            src_ref=piece(terms[i], (0, layer), block + 1 - k, h * 2 + q),
                            dst_ref=oth.at[slot, j, q],
                            send_sem=oth_send.at[slot, late],
                            recv_sem=oth_recv.at[slot, late],
                            device_id=partner,
                            device_id_type=MESH,
                        ).start()
                        pltpu.make_async_copy(piece(terms[i], (0, layer), block + k, h * 2 + q), own.at[slot, j, q], own_sem.at[slot, late]).start()

        for_weight(c, start)

    def load_old(c):
        slot = lax.rem(c, 2)

        def start(i, layer, h):
            for q in range(2):
                p = h * 2 + q
                pltpu.make_async_copy(piece(ms[i], (layer,), 0, p), m_in.at[slot, q], old_sem.at[slot, 0]).start()
                pltpu.make_async_copy(piece(vs[i], (layer,), 0, p), v_in.at[slot, q], old_sem.at[slot, 1]).start()
                pltpu.make_async_copy(piece(old[i], (layer,), me, p), w_in.at[slot, q], old_sem.at[slot, 2]).start()

        for_weight(c, start)

    def wait_for(ref, sem):
        pltpu.make_async_copy(ref, ref, sem).wait()

    def wait_terms(slot, late):
        part = pl.ds(late, 3) if late else pl.ds(0, 1)
        wait_for(own.at[slot, part], own_sem.at[slot, late])
        wait_for(oth.at[slot, part], oth_recv.at[slot, late])
        wait_for(oth.at[slot, part], oth_send.at[slot, late])

    def strips(body):
        @pl.loop(0, rows // STRIP)
        def _(r):
            body(pl.ds(pl.multiple_of(r * STRIP, STRIP), STRIP))

    def pair(slot, j, q, at):
        return own[slot, j, q, at].astype(jnp.float32) + oth[slot, j, q, at].astype(jnp.float32)

    def far_copy(c, q):
        return pltpu.make_async_remote_copy(
            src_ref=far.at[lax.rem(c, 2), q],
            dst_ref=from_far.at[c, q],
            send_sem=far_send.at[lax.rem(c, 2), q],
            recv_sem=far_recv.at[c, q],
            device_id=(right, left)[q],
            device_id_type=MESH,
        )

    def near_copy(c, d):
        return pltpu.make_async_remote_copy(
            src_ref=near.at[lax.rem(c, 2), d],
            dst_ref=from_near.at[c, d],
            send_sem=near_send.at[lax.rem(c, 2), d],
            recv_sem=near_recv.at[c, d],
            device_id=(right, left)[d],
            device_id_type=MESH,
        )

    def send_far(c):
        slot = lax.rem(c, 4)
        wait_terms(slot, 0)

        @pl.when(c >= 2)
        def _():
            for q in range(2):
                far_copy(c - 2, q).wait_send()

        def strip(at):
            for q in range(2):
                far[lax.rem(c, 2), q, at] = pair(slot, 0, q, at).astype(far.dtype)

        strips(strip)
        for q in range(2):
            far_copy(c, q).start()

    def send_near(c):
        slot = lax.rem(c, 4)
        wait_terms(slot, 1)

        @pl.when(c >= 2)
        def _():
            for d in range(2):
                near_copy(c - 2, d).wait_send()

        for q in range(2):
            far_copy(c, q).wait_recv()

        def strip(at):
            for d in range(2):
                for q in range(2):
                    total = pair(slot, 1 + d, q, at)
                    if q == d:
                        total += from_far[c, q, at].astype(jnp.float32)
                    near[lax.rem(c, 2), d, q, at] = total.astype(near.dtype)

        strips(strip)
        for d in range(2):
            near_copy(c, d).start()

    def outputs(c, act, act_remote):
        slot = lax.rem(c, 2)

        def go(i, layer, h):
            for q in range(2):
                p = h * 2 + q
                act(pltpu.make_async_copy(g_out.at[slot, q], piece(grads[i], (layer,), 0, p), out_sem.at[slot, q, 0]))
                for u, (weight, start, size) in enumerate(parts):
                    if weight == i:

                        @pl.when((layer >= start) & (layer < start + size))
                        def _():
                            act(pltpu.make_async_copy(w_out.at[slot, q], piece(fresh[u], (layer - start,), 0, p), out_sem.at[slot, q, 1]))
                            act_remote(
                                pltpu.make_async_remote_copy(
                                    src_ref=w_out.at[slot, q],
                                    dst_ref=piece(other[u], (layer - start,), 0, p),
                                    send_sem=other_send.at[slot, q],
                                    recv_sem=other_recv.at[u],
                                    device_id=partner,
                                    device_id_type=MESH,
                                )
                            )

        for_weight(c, go)

    def start_outputs(c):
        outputs(c, lambda copy: copy.start(), lambda copy: copy.start())

    def wait_outputs(c):
        outputs(c, lambda copy: copy.wait(), lambda copy: copy.wait_send())

    def first_copy(d):
        return pltpu.make_async_remote_copy(
            src_ref=fresh[0],
            dst_ref=first[d],
            send_sem=first_send.at[d],
            recv_sem=first_recv.at[d],
            device_id=(right, left)[d],
            device_id_type=MESH,
        )

    def finish(c):
        slot, two = lax.rem(c, 4), lax.rem(c, 2)
        wait_for(m_in.at[two], old_sem.at[two, 0])
        wait_for(v_in.at[two], old_sem.at[two, 1])
        wait_for(w_in.at[two], old_sem.at[two, 2])

        @pl.when(c >= 2)
        def _():
            wait_outputs(c - 2)

        for d in range(2):
            near_copy(c, d).wait_recv()

        def strip(at):
            for q in range(2):
                total = pair(slot, 3, q, at) + from_near[c, 0, q, at].astype(jnp.float32) + from_near[c, 1, q, at].astype(jnp.float32)
                g = total.astype(g_out.dtype)
                g_out[two, q, at] = g
                g = g.astype(jnp.float32)
                w = w_in[two, q, at].astype(jnp.float32)
                m = 0.9 * m_in[two, q, at] + 0.1 * g
                v = 0.95 * v_in[two, q, at] + 0.05 * g * g
                w_out[two, q, at] = (w - 0.02 * (m * lax.rsqrt(v + 1e-8) + 0.1 * w)).astype(w_out.dtype)

        strips(strip)
        start_outputs(c)

        @pl.when(c + 4 < chunks)
        def _():
            pl.semaphore_signal(free_sem, inc=1, device_id=partner, device_id_type=MESH)

    @pl.loop(0, chunks + 3)
    def _(s):
        @pl.when((s >= 1) & (s < chunks + 1))
        def _():
            send_far(s - 1)

        @pl.when(s < chunks)
        def _():
            @pl.when(s >= 4)
            def _():
                pl.semaphore_wait(free_sem, 1)

            load(s)

        @pl.when((s >= 2) & (s < chunks + 2))
        def _():
            load_old(s - 2)
            send_near(s - 2)

        @pl.when(s == chunks + 1)
        def _():
            for d in range(2):
                first_copy(d).start()

        @pl.when(s >= 3)
        def _():
            finish(s - 3)

    for c in (chunks - 2, chunks - 1):
        for q in range(2):
            far_copy(c, q).wait_send()
            near_copy(c, q).wait_send()
        wait_outputs(c)
    for u in range(count):
        wait_for(other[u], other_recv.at[u])
    for d in range(2):
        first_copy(d).wait()


def reduce_and_step(chips, parts, terms, weights, ms, vs):
    layers = terms[0].shape[1]
    chunks = 3 * layers * 2
    blocks = [jax.ShapeDtypeStruct((size, *ms[i].shape[1:]), jnp.bfloat16) for i, _, size in parts]
    rows, columns = min(m.shape[1] for m in ms), min(m.shape[2] for m in ms)
    bf, f32 = jnp.bfloat16, jnp.float32
    tile = (rows, columns)
    dma = pltpu.SemaphoreType.DMA
    out = pl.pallas_call(
        functools.partial(reduce_kernel, chips, layers, parts),
        out_shape=blocks * 2 + [jax.ShapeDtypeStruct(m.shape, bf) for m in ms] + blocks[:1] * 2,
        in_specs=[pl.BlockSpec(memory_space=pl.ANY)] * 12,
        out_specs=[pl.BlockSpec(memory_space=pl.ANY)] * (2 * len(parts) + 5),
        scratch_shapes=[
            pltpu.VMEM((4, 4, 2, *tile), bf),
            pltpu.VMEM((4, 4, 2, *tile), bf),
            pltpu.VMEM((2, 2, *tile), f32),
            pltpu.VMEM((2, 2, *tile), f32),
            pltpu.VMEM((2, 2, *tile), bf),
            pltpu.VMEM((2, 2, *tile), bf),
            pltpu.VMEM((2, 2, *tile), bf),
            pltpu.VMEM((2, 2, *tile), bf),
            pltpu.VMEM((2, 2, 2, *tile), bf),
            pltpu.VMEM((chunks, 2, *tile), bf),
            pltpu.VMEM((chunks, 2, 2, *tile), bf),
            dma((4, 2)),
            dma((4, 2)),
            dma((4, 2)),
            dma((2, 3)),
            dma((2, 2, 2)),
            dma((2, 2)),
            dma((chunks, 2)),
            dma((2, 2)),
            dma((chunks, 2)),
            dma((2, 2)),
            dma((len(parts),)),
            dma((2,)),
            dma((2,)),
            pltpu.SemaphoreType.REGULAR,
        ],
        compiler_params=pltpu.CompilerParams(collective_id=0, has_side_effects=True, vmem_limit_bytes=67_000_000),
        name="reduce",
    )(*terms, *weights, *ms, *vs)
    count = len(parts)
    return out[:count], out[count : 2 * count], list(out[2 * count : 2 * count + 3]), out[-2:]


def place_kernel(chips, jobs, *refs):
    out, buf, in_sem, out_sem = refs[-4:]
    me = lax.axis_index("dp")
    x, k = me // CORES, lax.rem(me, CORES)
    copies = []
    for i, (layer, layers, rows, step, at, block_rows, other) in enumerate(jobs):
        block = lax.rem(x + step, chips) * CORES + (1 - k if other else k)
        slot = buf.at[i, pl.ds(0, layers), pl.ds(0, rows)]
        into = out.at[pl.ds(layer, layers), pl.ds(pl.multiple_of(block * block_rows + at, 8), rows)]
        copies.append((pltpu.make_async_copy(refs[i], slot, in_sem.at[i]), pltpu.make_async_copy(slot, into, out_sem.at[i])))
        copies[i][0].start()
    for first, second in copies:
        first.wait()
        second.start()
    for _, second in copies:
        second.wait()


def place(chips, shape, pieces, so_far):
    arrays = [p[0] for p in pieces]
    jobs = [(p[1], *p[0].shape[:2], *p[2:]) for p in pieces]
    size = max(a.shape[0] for a in arrays), max(a.shape[1] for a in arrays), arrays[0].shape[2]
    extra = () if so_far is None else (so_far,)
    return pl.pallas_call(
        functools.partial(place_kernel, chips, jobs),
        out_shape=jax.ShapeDtypeStruct(shape, jnp.bfloat16),
        in_specs=[pl.BlockSpec(memory_space=pl.ANY)] * (len(jobs) + len(extra)),
        out_specs=pl.BlockSpec(memory_space=pl.ANY),
        scratch_shapes=[
            pltpu.VMEM((len(jobs), *size), jnp.bfloat16),
            pltpu.SemaphoreType.DMA((len(jobs),)),
            pltpu.SemaphoreType.DMA((len(jobs),)),
        ],
        input_output_aliases={len(jobs): 0} if extra else {},
        compiler_params=pltpu.CompilerParams(vmem_limit_bytes=67_000_000),
        cost_estimate=pl.CostEstimate(flops=20_000_000, bytes_accessed=4 * sum(a.size for a in arrays), transcendentals=0),
        name="place",
    )(*arrays, *extra)


def solution(mesh):
    n = mesh.shape["dp"]
    chips = n // CORES

    def pairs(step, flip=0):
        return [(x * CORES + k, (x + step) % chips * CORES + (k + flip) % CORES) for x in range(chips) for k in range(CORES)]

    right, left, partner = pairs(1), pairs(-1), pairs(0, 1)

    def send(a, where):
        return lax.ppermute(a, "dp", where)

    def step(*arrays):
        terms, weights, ms, vs = (arrays[i : i + 3] for i in (0, 3, 6, 9))
        layers = terms[0].shape[1]
        f32 = jnp.float32
        parts = [(i, 0, layers) for i in range(2)] + [(2, layer, 1) for layer in range(layers)]
        fresh, other, gradients, first = reduce_and_step(chips, parts, terms, weights, ms, vs)

        last = len(parts) - 1
        whole, new_m, new_v = [None] * 3, [None] * 3, [None] * 3
        near, far, cuts = {0: first}, {}, {}
        for at, (i, start, size) in enumerate(parts):
            if at:
                near[at] = send(fresh[at], right), send(fresh[at], left)
            a, b = near[at]
            by_layer = size % 2 == 0
            half = (size if by_layer else a.shape[1]) // 2
            c, d = (a[:half], b[half:]) if by_layer else (a[:, :half], b[:, half:])
            cuts[at] = (start, 0), (start + half, 0) if by_layer else (start, half)
            far[at] = send(c, right), send(d, left)

        def put(at, pieces, apart=False):
            i = parts[at][0]
            rows = fresh[at].shape[1]
            theirs = [send(a, partner) if p is None else p for a, p, *_ in pieces]
            mine = [(p[0], *p[2:], rows, False) for p in pieces]
            theirs = [(t, *p[2:], rows, True) for t, p in zip(theirs, pieces)]
            if apart:
                whole[i] = place(chips, weights[i].shape, mine, whole[i])
                mine = []
            whole[i] = place(chips, weights[i].shape, mine + theirs, whole[i])

        for w in range(1, 3):
            c, d = far[w - 1]
            gradients[w], c = lax.optimization_barrier((gradients[w], c))
            far[w - 1] = c, d

        def put_far(at, apart=False):
            (c, d), ((c_layer, c_row), (d_layer, d_row)) = far[at], cuts[at]
            put(at, [(c, None, c_layer, 2, c_row), (d, None, d_layer, 2, d_row)], apart)

        for at, (i, start, _) in enumerate(parts):
            a, b = near[at]
            put(at, [(fresh[at], other[at], start, 0, 0), (a, None, start, chips - 1, 0), (b, None, start, 1, 0)])
            if at:
                put_far(at - 1)
        put_far(last, apart=True)
        for w in range(3):
            g = gradients[w].astype(f32)
            new_m[w] = 0.9 * ms[w] + 0.1 * g
            new_v[w] = 0.95 * vs[w] + 0.05 * g * g
        return (*whole, *new_m, *new_v)

    all_of, cut = P(None, None, None), P(None, "dp", None)
    return jax.shard_map(
        step,
        mesh=mesh,
        in_specs=(P(("rep", "dp"), None, None, None),) * 3 + (all_of,) * 3 + (cut,) * 6,
        out_specs=(P("rep", None, None),) * 3 + (P("rep", "dp", None),) * 6,
        check_vma=False,
    )
```

```python
import functools

import jax
import jax.numpy as jnp
from jax import lax
from jax.experimental import pallas as pl
from jax.experimental.pallas import tpu as pltpu
from jax.sharding import PartitionSpec as P


CORES = 2
PIECES = 4
STRIP = 16
SLOTS = 4
GROUPS = 3
MESH = pl.DeviceIdType.MESH
ORDER = (2, 1, 3, 0)


def reduce_kernel(chips, layers, parts, *refs):
    weights = 3
    terms, old, ms, vs = (refs[i : i + weights] for i in range(0, 4 * weights, weights))
    units = weights * layers
    count = len(parts)
    outs = refs[4 * weights : 5 * weights + 2 * count + 2]
    fresh, other, grads = outs[:count], outs[count : 2 * count], outs[2 * count : 2 * count + weights]
    first = outs[-2:]
    (own, oth, m_in, v_in, w_in, w_out, g_out, far, near, from_far, from_near,
     own_sem, oth_send, oth_recv, old_sem, out_sem, far_send, far_recv, near_send, near_recv,
     other_send, other_recv, first_send, first_recv, free_sem) = refs[5 * weights + 2 * count + 2 :]
    rows, columns = own.shape[-2:]
    chunks = units * 2
    me = lax.axis_index("dp")
    x, k = me // CORES, lax.rem(me, CORES)
    right = {"dp": lax.rem(x + 1, chips) * CORES + k}
    left = {"dp": lax.rem(x + chips - 1, chips) * CORES + k}
    partner = {"dp": x * CORES + 1 - k}

    barrier = pltpu.get_barrier_semaphore()
    for who in (right, left, partner):
        pl.semaphore_signal(barrier, inc=1, device_id=who, device_id_type=MESH)
    pl.semaphore_wait(barrier, 3)

    def piece(ref, lead, block, p):
        if ref.shape[-1] == columns:
            return ref.at[(*lead, pl.ds(pl.multiple_of((block * PIECES + p) * rows, 8), rows))]
        return ref.at[(*lead, pl.ds(pl.multiple_of(block * rows, 8), rows), pl.ds(pl.multiple_of(p * columns, 128), columns))]

    def for_weight(c, body):
        for i in range(weights):
            pl.when(c // (layers * 2) == i)(functools.partial(body, i, lax.rem(c // 2, layers), lax.rem(c, 2)))

    def load(c, group, cuts):
        slot = lax.rem(c, SLOTS)
        size = rows // cuts

        def start(i, layer, h):
            for r in range(cuts):
                at = pl.ds(r * size, size)
                sem = r if 0 in group else GROUPS
                for j in group:
                    block = lax.rem(x + ORDER[j], chips) * CORES
                    for q in range(2):
                        pltpu.make_async_remote_copy(
                            src_ref=piece(terms[i], (0, layer), block + 1 - k, h * 2 + q).at[at],
                            dst_ref=oth.at[slot, j, q, at],
                            send_sem=oth_send.at[slot, sem],
                            recv_sem=oth_recv.at[slot, sem],
                            device_id=partner,
                            device_id_type=MESH,
                        ).start()
                        pltpu.make_async_copy(piece(terms[i], (0, layer), block + k, h * 2 + q).at[at], own.at[slot, j, q, at], own_sem.at[slot, sem]).start()

        for_weight(c, start)

    def load_far(c):
        load(c, (0,), GROUPS)

    def load_near(c):
        load(c, (1, 2, 3), 1)

    def load_old(c):
        slot = lax.rem(c, 2)

        def start(i, layer, h):
            for q in range(2):
                p = h * 2 + q
                pltpu.make_async_copy(piece(ms[i], (layer,), 0, p), m_in.at[slot, q], old_sem.at[slot, 0]).start()
                pltpu.make_async_copy(piece(vs[i], (layer,), 0, p), v_in.at[slot, q], old_sem.at[slot, 1]).start()
                pltpu.make_async_copy(piece(old[i], (layer,), me, p), w_in.at[slot, q], old_sem.at[slot, 2]).start()

        for_weight(c, start)

    def wait_for(ref, sem):
        pltpu.make_async_copy(ref, ref, sem).wait()

    def wait_terms(slot, part, at, sem):
        wait_for(own.at[slot, part, :, at], own_sem.at[slot, sem])
        wait_for(oth.at[slot, part, :, at], oth_recv.at[slot, sem])
        wait_for(oth.at[slot, part, :, at], oth_send.at[slot, sem])

    def strips(body, first=0, count=rows):
        @pl.loop(0, count // STRIP)
        def _(r):
            body(pl.ds(pl.multiple_of(first + r * STRIP, STRIP), STRIP))

    def pair(slot, j, q, at):
        return own[slot, j, q, at].astype(jnp.float32) + oth[slot, j, q, at].astype(jnp.float32)

    def far_copy(c, q, at=pl.ds(0, rows)):
        return pltpu.make_async_remote_copy(
            src_ref=far.at[lax.rem(c, 2), q, at],
            dst_ref=from_far.at[c, q, at],
            send_sem=far_send.at[lax.rem(c, 2), q],
            recv_sem=far_recv.at[c, q],
            device_id=(right, left)[q],
            device_id_type=MESH,
        )

    def near_copy(c, d):
        return pltpu.make_async_remote_copy(
            src_ref=near.at[lax.rem(c, 2), d],
            dst_ref=from_near.at[c, d],
            send_sem=near_send.at[lax.rem(c, 2), d],
            recv_sem=near_recv.at[c, d],
            device_id=(right, left)[d],
            device_id_type=MESH,
        )

    def send_far(c):
        slot = lax.rem(c, SLOTS)

        @pl.when(c >= 2)
        def _():
            for q in range(2):
                far_copy(c - 2, q).wait_send()

        def strip(at):
            for q in range(2):
                far[lax.rem(c, 2), q, at] = pair(slot, 0, q, at).astype(far.dtype)

        size = rows // GROUPS
        for r in range(GROUPS):
            at = pl.ds(r * size, size)
            wait_terms(slot, pl.ds(0, 1), at, r)
            strips(strip, r * size, size)
            for q in range(2):
                far_copy(c, q, at).start()

    def send_near(c):
        slot = lax.rem(c, SLOTS)
        wait_terms(slot, pl.ds(1, 3), pl.ds(0, rows), GROUPS)

        @pl.when(c >= 2)
        def _():
            for d in range(2):
                near_copy(c - 2, d).wait_send()

        for q in range(2):
            far_copy(c, q).wait_recv()

        def strip(at):
            for d in range(2):
                for q in range(2):
                    total = pair(slot, 1 + d, q, at)
                    if q == d:
                        total += from_far[c, q, at].astype(jnp.float32)
                    near[lax.rem(c, 2), d, q, at] = total.astype(near.dtype)

        strips(strip)
        for d in range(2):
            near_copy(c, d).start()

    def outputs(c, act, act_remote):
        slot = lax.rem(c, 2)

        def go(i, layer, h):
            for q in range(2):
                p = h * 2 + q
                act(pltpu.make_async_copy(g_out.at[slot, q], piece(grads[i], (layer,), 0, p), out_sem.at[slot, q, 0]))
                for u, (weight, start, size) in enumerate(parts):
                    if weight == i:

                        @pl.when((layer >= start) & (layer < start + size))
                        def _():
                            act(pltpu.make_async_copy(w_out.at[slot, q], piece(fresh[u], (layer - start,), 0, p), out_sem.at[slot, q, 1]))
                            act_remote(
                                pltpu.make_async_remote_copy(
                                    src_ref=w_out.at[slot, q],
                                    dst_ref=piece(other[u], (layer - start,), 0, p),
                                    send_sem=other_send.at[slot, q],
                                    recv_sem=other_recv.at[u],
                                    device_id=partner,
                                    device_id_type=MESH,
                                )
                            )

        for_weight(c, go)

    def start_outputs(c):
        outputs(c, lambda copy: copy.start(), lambda copy: copy.start())

    def wait_outputs(c):
        outputs(c, lambda copy: copy.wait(), lambda copy: copy.wait_send())

    def first_copy(d):
        return pltpu.make_async_remote_copy(
            src_ref=fresh[0],
            dst_ref=first[d],
            send_sem=first_send.at[d],
            recv_sem=first_recv.at[d],
            device_id={"dp": lax.rem(x + (chips - 1 if d else 1) * (1 - 2 * k) + chips, chips) * CORES + k},
            device_id_type=MESH,
        )

    def finish(c):
        slot, two = lax.rem(c, SLOTS), lax.rem(c, 2)
        wait_for(m_in.at[two], old_sem.at[two, 0])
        wait_for(v_in.at[two], old_sem.at[two, 1])
        wait_for(w_in.at[two], old_sem.at[two, 2])

        @pl.when(c >= 2)
        def _():
            wait_outputs(c - 2)

        for d in range(2):
            near_copy(c, d).wait_recv()

        def strip(at):
            for q in range(2):
                total = pair(slot, 3, q, at) + from_near[c, 0, q, at].astype(jnp.float32) + from_near[c, 1, q, at].astype(jnp.float32)
                g = total.astype(g_out.dtype)
                g_out[two, q, at] = g
                g = g.astype(jnp.float32)
                w = w_in[two, q, at].astype(jnp.float32)
                m = 0.9 * m_in[two, q, at] + 0.1 * g
                v = 0.95 * v_in[two, q, at] + 0.05 * g * g
                w_out[two, q, at] = (w - 0.02 * (m * lax.rsqrt(v + 1e-8) + 0.1 * w)).astype(w_out.dtype)

        strips(strip)
        start_outputs(c)

        @pl.when(c + SLOTS < chunks)
        def _():
            pl.semaphore_signal(free_sem, inc=1, device_id=partner, device_id_type=MESH)

    @pl.loop(0, chunks + 3)
    def _(s):
        @pl.when((s >= 1) & (s < chunks + 1))
        def _():
            send_far(s - 1)
            load_near(s - 1)

        @pl.when(s < chunks)
        def _():
            @pl.when(s >= SLOTS)
            def _():
                pl.semaphore_wait(free_sem, 1)

            load_far(s)

        @pl.when((s >= 2) & (s < chunks + 2))
        def _():
            load_old(s - 2)
            send_near(s - 2)

        @pl.when((s == chunks + 1) & (k == 0))
        def _():
            for d in range(2):
                first_copy(d).start()

        @pl.when(s >= 3)
        def _():
            finish(s - 3)

    for c in (chunks - 2, chunks - 1):
        for q in range(2):
            far_copy(c, q).wait_send()
            near_copy(c, q).wait_send()
        wait_outputs(c)

    @pl.when(k != 0)
    def _():
        for d in range(2):
            first_copy(d).start()

    for u in range(count):
        wait_for(other[u], other_recv.at[u])
    for d in range(2):
        first_copy(d).wait()


def reduce_and_step(chips, parts, terms, weights, ms, vs):
    layers = terms[0].shape[1]
    chunks = 3 * layers * 2
    blocks = [jax.ShapeDtypeStruct((size, *ms[i].shape[1:]), jnp.bfloat16) for i, _, size in parts]
    rows, columns = min(m.shape[1] for m in ms), min(m.shape[2] for m in ms)
    bf, f32 = jnp.bfloat16, jnp.float32
    tile = (rows, columns)
    dma = pltpu.SemaphoreType.DMA
    out = pl.pallas_call(
        functools.partial(reduce_kernel, chips, layers, parts),
        out_shape=blocks * 2 + [jax.ShapeDtypeStruct(m.shape, bf) for m in ms] + blocks[:1] * 2,
        in_specs=[pl.BlockSpec(memory_space=pl.ANY)] * 12,
        out_specs=[pl.BlockSpec(memory_space=pl.ANY)] * (2 * len(parts) + 5),
        scratch_shapes=[
            pltpu.VMEM((SLOTS, 4, 2, *tile), bf),
            pltpu.VMEM((SLOTS, 4, 2, *tile), bf),
            pltpu.VMEM((2, 2, *tile), f32),
            pltpu.VMEM((2, 2, *tile), f32),
            pltpu.VMEM((2, 2, *tile), bf),
            pltpu.VMEM((2, 2, *tile), bf),
            pltpu.VMEM((2, 2, *tile), bf),
            pltpu.VMEM((2, 2, *tile), bf),
            pltpu.VMEM((2, 2, 2, *tile), bf),
            pltpu.VMEM((chunks, 2, *tile), bf),
            pltpu.VMEM((chunks, 2, 2, *tile), bf),
            dma((SLOTS, GROUPS + 1)),
            dma((SLOTS, GROUPS + 1)),
            dma((SLOTS, GROUPS + 1)),
            dma((2, 3)),
            dma((2, 2, 2)),
            dma((2, 2)),
            dma((chunks, 2)),
            dma((2, 2)),
            dma((chunks, 2)),
            dma((2, 2)),
            dma((len(parts),)),
            dma((2,)),
            dma((2,)),
            pltpu.SemaphoreType.REGULAR,
        ],
        compiler_params=pltpu.CompilerParams(collective_id=0, has_side_effects=True, vmem_limit_bytes=67_000_000),
        name="reduce",
    )(*terms, *weights, *ms, *vs)
    count = len(parts)
    return out[:count], out[count : 2 * count], list(out[2 * count : 2 * count + 3]), out[-2:]


def place_kernel(chips, jobs, *refs):
    out, buf, in_sem, out_sem = refs[-4:]
    me = lax.axis_index("dp")
    x, k = me // CORES, lax.rem(me, CORES)
    copies = []
    for i, (layer, layers, rows, step, at, block_rows, other) in enumerate(jobs):
        core = 1 - k if other else k
        block = lax.rem(x + step * (1 - 2 * core) + chips, chips) * CORES + core
        slot = buf.at[i, pl.ds(0, layers), pl.ds(0, rows)]
        into = out.at[pl.ds(layer, layers), pl.ds(pl.multiple_of(block * block_rows + at, 8), rows)]
        copies.append((pltpu.make_async_copy(refs[i], slot, in_sem.at[i]), pltpu.make_async_copy(slot, into, out_sem.at[i])))
        copies[i][0].start()
    for first, second in copies:
        first.wait()
        second.start()
    for _, second in copies:
        second.wait()


def place(chips, shape, pieces, so_far):
    arrays = [p[0] for p in pieces]
    jobs = [(p[1], *p[0].shape[:2], *p[2:]) for p in pieces]
    size = max(a.shape[0] for a in arrays), max(a.shape[1] for a in arrays), arrays[0].shape[2]
    extra = () if so_far is None else (so_far,)
    return pl.pallas_call(
        functools.partial(place_kernel, chips, jobs),
        out_shape=jax.ShapeDtypeStruct(shape, jnp.bfloat16),
        in_specs=[pl.BlockSpec(memory_space=pl.ANY)] * (len(jobs) + len(extra)),
        out_specs=pl.BlockSpec(memory_space=pl.ANY),
        scratch_shapes=[
            pltpu.VMEM((len(jobs), *size), jnp.bfloat16),
            pltpu.SemaphoreType.DMA((len(jobs),)),
            pltpu.SemaphoreType.DMA((len(jobs),)),
        ],
        input_output_aliases={len(jobs): 0} if extra else {},
        compiler_params=pltpu.CompilerParams(vmem_limit_bytes=67_000_000),
        cost_estimate=pl.CostEstimate(flops=20_000_000, bytes_accessed=4 * sum(a.size for a in arrays), transcendentals=0),
        name="place",
    )(*arrays, *extra)


def solution(mesh):
    n = mesh.shape["dp"]
    chips = n // CORES

    def pairs(step, flip=0):
        return [(x * CORES + k, (x + step * (1 - 2 * k)) % chips * CORES + (k + flip) % CORES) for x in range(chips) for k in range(CORES)]

    one_way, other_way, partner = pairs(1), pairs(-1), pairs(0, 1)

    def send(a, where):
        return lax.ppermute(a, "dp", where)

    def step(*arrays):
        terms, weights, ms, vs = (arrays[i : i + 3] for i in (0, 3, 6, 9))
        layers = terms[0].shape[1]
        f32 = jnp.float32
        parts = [(i, 0, layers) for i in range(2)] + [(2, layer, 1) for layer in range(layers)]
        fresh, other, gradients, first = reduce_and_step(chips, parts, terms, weights, ms, vs)

        last = len(parts) - 1
        whole, new_m, new_v = [None] * 3, [None] * 3, [None] * 3
        near, far, cuts = {0: first}, {}, {}
        for at, (i, start, size) in enumerate(parts):
            if at:
                near[at] = send(fresh[at], one_way), send(fresh[at], other_way)
            a, b = near[at]
            by_layer = size % 2 == 0
            half = (size if by_layer else a.shape[1]) // 2
            c, d = (a[:half], b[half:]) if by_layer else (a[:, :half], b[:, half:])
            cuts[at] = (start, 0), (start + half, 0) if by_layer else (start, half)
            far[at] = send(c, one_way), send(d, other_way)

        def put(at, pieces, apart=False):
            i = parts[at][0]
            rows = fresh[at].shape[1]
            theirs = [send(a, partner) if p is None else p for a, p, *_ in pieces]
            mine = [(p[0], *p[2:], rows, False) for p in pieces]
            theirs = [(t, *p[2:], rows, True) for t, p in zip(theirs, pieces)]
            if apart:
                whole[i] = place(chips, weights[i].shape, mine, whole[i])
                mine = []
            whole[i] = place(chips, weights[i].shape, mine + theirs, whole[i])

        for w in range(1, 3):
            c, d = far[w - 1]
            gradients[w], c = lax.optimization_barrier((gradients[w], c))
            far[w - 1] = c, d

        def put_far(at, apart=False):
            (c, d), ((c_layer, c_row), (d_layer, d_row)) = far[at], cuts[at]
            put(at, [(c, None, c_layer, 2, c_row), (d, None, d_layer, 2, d_row)], apart)

        for at, (i, start, _) in enumerate(parts):
            a, b = near[at]
            put(at, [(fresh[at], other[at], start, 0, 0), (a, None, start, chips - 1, 0), (b, None, start, 1, 0)])
            if at:
                put_far(at - 1)
        put_far(last, apart=True)
        for w in range(3):
            g = gradients[w].astype(f32)
            new_m[w] = 0.9 * ms[w] + 0.1 * g
            new_v[w] = 0.95 * vs[w] + 0.05 * g * g
        return (*whole, *new_m, *new_v)

    all_of, cut = P(None, None, None), P(None, "dp", None)
    return jax.shard_map(
        step,
        mesh=mesh,
        in_specs=(P(("rep", "dp"), None, None, None),) * 3 + (all_of,) * 3 + (cut,) * 6,
        out_specs=(P("rep", None, None),) * 3 + (P("rep", "dp", None),) * 6,
        check_vma=False,
    )
```

```python
import functools

import jax
import jax.numpy as jnp
from jax import lax
from jax.experimental import pallas as pl
from jax.experimental.pallas import tpu as pltpu
from jax.sharding import PartitionSpec as P


CORES = 2
PIECES = 4
STRIP = 16
SLOTS = 4
GROUPS = 3
EARLY = (2, 3)
MESH = pl.DeviceIdType.MESH
ORDER = (2, 1, 3, 0)


def reduce_kernel(chips, layers, parts, *refs):
    weights = 3
    terms, old, ms, vs = (refs[i : i + weights] for i in range(0, 4 * weights, weights))
    units = weights * layers
    count = len(parts)
    outs = refs[4 * weights : 5 * weights + 2 * count + 2]
    fresh, other, grads = outs[:count], outs[count : 2 * count], outs[2 * count : 2 * count + weights]
    first = outs[-2:]
    (own, oth, m_in, v_in, w_in, w_out, g_out, far, near, from_far, from_near,
     own_sem, oth_send, oth_recv, old_sem, out_sem, far_send, far_recv, near_send, near_recv,
     other_send, other_recv, first_send, first_recv, free_sem) = refs[5 * weights + 2 * count + 2 :]
    rows, columns = own.shape[-2:]
    chunks = units * 2
    me = lax.axis_index("dp")
    x, k = me // CORES, lax.rem(me, CORES)
    right = {"dp": lax.rem(x + 1, chips) * CORES + k}
    left = {"dp": lax.rem(x + chips - 1, chips) * CORES + k}
    partner = {"dp": x * CORES + 1 - k}

    barrier = pltpu.get_barrier_semaphore()
    for who in (right, left, partner):
        pl.semaphore_signal(barrier, inc=1, device_id=who, device_id_type=MESH)
    pl.semaphore_wait(barrier, 3)

    def piece(ref, lead, block, p):
        if ref.shape[-1] == columns:
            return ref.at[(*lead, pl.ds(pl.multiple_of((block * PIECES + p) * rows, 8), rows))]
        return ref.at[(*lead, pl.ds(pl.multiple_of(block * rows, 8), rows), pl.ds(pl.multiple_of(p * columns, 128), columns))]

    def for_weight(c, body):
        for i in range(weights):
            pl.when(c // (layers * 2) == i)(functools.partial(body, i, lax.rem(c // 2, layers), lax.rem(c, 2)))

    def load(c, group, cuts):
        slot = lax.rem(c, SLOTS)
        size = rows // cuts

        def start(i, layer, h):
            for r in range(cuts):
                at = pl.ds(r * size, size)
                sem = r if 0 in group else GROUPS
                for j in group:
                    block = lax.rem(x + ORDER[j], chips) * CORES
                    for q in range(2):
                        pltpu.make_async_remote_copy(
                            src_ref=piece(terms[i], (0, layer), block + 1 - k, h * 2 + q).at[at],
                            dst_ref=oth.at[slot, j, q, at],
                            send_sem=oth_send.at[slot, sem],
                            recv_sem=oth_recv.at[slot, sem],
                            device_id=partner,
                            device_id_type=MESH,
                        ).start()
                        pltpu.make_async_copy(piece(terms[i], (0, layer), block + k, h * 2 + q).at[at], own.at[slot, j, q, at], own_sem.at[slot, sem]).start()

        for_weight(c, start)

    def load_far(c):
        load(c, (0,), GROUPS)

    def load_near(c):
        load(c, (1, 2, 3), 1)

    def load_old(c):
        slot = lax.rem(c, 2)

        def start(i, layer, h):
            for q in range(2):
                p = h * 2 + q
                pltpu.make_async_copy(piece(ms[i], (layer,), 0, p), m_in.at[slot, q], old_sem.at[slot, 0]).start()
                pltpu.make_async_copy(piece(vs[i], (layer,), 0, p), v_in.at[slot, q], old_sem.at[slot, 1]).start()
                pltpu.make_async_copy(piece(old[i], (layer,), me, p), w_in.at[slot, q], old_sem.at[slot, 2]).start()

        for_weight(c, start)

    def wait_for(ref, sem):
        pltpu.make_async_copy(ref, ref, sem).wait()

    def wait_terms(slot, part, at, sem):
        wait_for(own.at[slot, part, :, at], own_sem.at[slot, sem])
        wait_for(oth.at[slot, part, :, at], oth_recv.at[slot, sem])
        wait_for(oth.at[slot, part, :, at], oth_send.at[slot, sem])

    def strips(body, first=0, count=rows):
        @pl.loop(0, count // STRIP)
        def _(r):
            body(pl.ds(pl.multiple_of(first + r * STRIP, STRIP), STRIP))

    def pair(slot, j, q, at):
        return own[slot, j, q, at].astype(jnp.float32) + oth[slot, j, q, at].astype(jnp.float32)

    def far_copy(c, q, at=pl.ds(0, rows)):
        return pltpu.make_async_remote_copy(
            src_ref=far.at[lax.rem(c, 2), q, at],
            dst_ref=from_far.at[c, q, at],
            send_sem=far_send.at[lax.rem(c, 2), q],
            recv_sem=far_recv.at[c, q],
            device_id=(right, left)[q],
            device_id_type=MESH,
        )

    def near_copy(c, d):
        return pltpu.make_async_remote_copy(
            src_ref=near.at[lax.rem(c, 2), d],
            dst_ref=from_near.at[c, d],
            send_sem=near_send.at[lax.rem(c, 2), d],
            recv_sem=near_recv.at[c, d],
            device_id=(right, left)[d],
            device_id_type=MESH,
        )

    def send_far(c):
        slot = lax.rem(c, SLOTS)

        @pl.when(c >= 2)
        def _():
            for q in range(2):
                far_copy(c - 2, q).wait_send()

        def strip(at):
            for q in range(2):
                far[lax.rem(c, 2), q, at] = pair(slot, 0, q, at).astype(far.dtype)

        size = rows // GROUPS
        for r in range(GROUPS):
            at = pl.ds(r * size, size)
            wait_terms(slot, pl.ds(0, 1), at, r)
            strips(strip, r * size, size)
            for q in range(2):
                far_copy(c, q, at).start()

    def send_near(c):
        slot = lax.rem(c, SLOTS)
        wait_terms(slot, pl.ds(1, 3), pl.ds(0, rows), GROUPS)

        @pl.when(c >= 2)
        def _():
            for d in range(2):
                near_copy(c - 2, d).wait_send()

        for q in range(2):
            far_copy(c, q).wait_recv()

        def strip(at):
            for d in range(2):
                for q in range(2):
                    total = pair(slot, 1 + d, q, at)
                    if q == d:
                        total += from_far[c, q, at].astype(jnp.float32)
                    near[lax.rem(c, 2), d, q, at] = total.astype(near.dtype)

        strips(strip)
        for d in range(2):
            near_copy(c, d).start()

    def outputs(c, act, act_remote):
        slot = lax.rem(c, 2)

        def go(i, layer, h):
            for q in range(2):
                p = h * 2 + q
                act(pltpu.make_async_copy(g_out.at[slot, q], piece(grads[i], (layer,), 0, p), out_sem.at[slot, q, 0]))
                for u, (weight, start, size) in enumerate(parts):
                    if weight == i:

                        @pl.when((layer >= start) & (layer < start + size))
                        def _():
                            act(pltpu.make_async_copy(w_out.at[slot, q], piece(fresh[u], (layer - start,), 0, p), out_sem.at[slot, q, 1]))
                            act_remote(
                                pltpu.make_async_remote_copy(
                                    src_ref=w_out.at[slot, q],
                                    dst_ref=piece(other[u], (layer - start,), 0, p),
                                    send_sem=other_send.at[slot, q],
                                    recv_sem=other_recv.at[u],
                                    device_id=partner,
                                    device_id_type=MESH,
                                )
                            )

        for_weight(c, go)

    def start_outputs(c):
        outputs(c, lambda copy: copy.start(), lambda copy: copy.start())

    def wait_outputs(c):
        outputs(c, lambda copy: copy.wait(), lambda copy: copy.wait_send())

    def first_copy(d):
        return pltpu.make_async_remote_copy(
            src_ref=fresh[0],
            dst_ref=first[d],
            send_sem=first_send.at[d],
            recv_sem=first_recv.at[d],
            device_id={"dp": lax.rem(x + (chips - 1 if d else 1) * (1 - 2 * k) + chips, chips) * CORES + k},
            device_id_type=MESH,
        )

    def finish(c):
        slot, two = lax.rem(c, SLOTS), lax.rem(c, 2)
        wait_for(m_in.at[two], old_sem.at[two, 0])
        wait_for(v_in.at[two], old_sem.at[two, 1])
        wait_for(w_in.at[two], old_sem.at[two, 2])

        @pl.when(c >= 2)
        def _():
            wait_outputs(c - 2)

        for d in range(2):
            near_copy(c, d).wait_recv()

        def strip(at):
            for q in range(2):
                total = pair(slot, 3, q, at) + from_near[c, 0, q, at].astype(jnp.float32) + from_near[c, 1, q, at].astype(jnp.float32)
                g = total.astype(g_out.dtype)
                g_out[two, q, at] = g
                g = g.astype(jnp.float32)
                w = w_in[two, q, at].astype(jnp.float32)
                m = 0.9 * m_in[two, q, at] + 0.1 * g
                v = 0.95 * v_in[two, q, at] + 0.05 * g * g
                w_out[two, q, at] = (w - 0.02 * (m * lax.rsqrt(v + 1e-8) + 0.1 * w)).astype(w_out.dtype)

        strips(strip)
        start_outputs(c)

        @pl.when(c + SLOTS < chunks)
        def _():
            pl.semaphore_signal(free_sem, inc=1, device_id=partner, device_id_type=MESH)

    @pl.loop(0, chunks + 3)
    def _(s):
        @pl.when((s >= 1) & (s < chunks + 1))
        def _():
            send_far(s - 1)
            load_near(s - 1)

        @pl.when(s < chunks)
        def _():
            @pl.when(s >= SLOTS)
            def _():
                pl.semaphore_wait(free_sem, 1)

            load_far(s)

        @pl.when((s >= 2) & (s < chunks + 2))
        def _():
            load_old(s - 2)
            send_near(s - 2)

        @pl.when((s == chunks + 1) & (k == 0))
        def _():
            for d in range(2):
                first_copy(d).start()

        @pl.when(s >= 3)
        def _():
            finish(s - 3)

    for c in (chunks - 2, chunks - 1):
        for q in range(2):
            far_copy(c, q).wait_send()
            near_copy(c, q).wait_send()
        wait_outputs(c)

    @pl.when(k != 0)
    def _():
        for d in range(2):
            first_copy(d).start()

    for u in range(count):
        wait_for(other[u], other_recv.at[u])
    for d in range(2):
        first_copy(d).wait()


def reduce_and_step(chips, parts, terms, weights, ms, vs):
    layers = terms[0].shape[1]
    chunks = 3 * layers * 2
    blocks = [jax.ShapeDtypeStruct((size, *ms[i].shape[1:]), jnp.bfloat16) for i, _, size in parts]
    rows, columns = min(m.shape[1] for m in ms), min(m.shape[2] for m in ms)
    bf, f32 = jnp.bfloat16, jnp.float32
    tile = (rows, columns)
    dma = pltpu.SemaphoreType.DMA
    out = pl.pallas_call(
        functools.partial(reduce_kernel, chips, layers, parts),
        out_shape=blocks * 2 + [jax.ShapeDtypeStruct(m.shape, bf) for m in ms] + blocks[:1] * 2,
        in_specs=[pl.BlockSpec(memory_space=pl.ANY)] * 12,
        out_specs=[pl.BlockSpec(memory_space=pl.ANY)] * (2 * len(parts) + 5),
        scratch_shapes=[
            pltpu.VMEM((SLOTS, 4, 2, *tile), bf),
            pltpu.VMEM((SLOTS, 4, 2, *tile), bf),
            pltpu.VMEM((2, 2, *tile), f32),
            pltpu.VMEM((2, 2, *tile), f32),
            pltpu.VMEM((2, 2, *tile), bf),
            pltpu.VMEM((2, 2, *tile), bf),
            pltpu.VMEM((2, 2, *tile), bf),
            pltpu.VMEM((2, 2, *tile), bf),
            pltpu.VMEM((2, 2, 2, *tile), bf),
            pltpu.VMEM((chunks, 2, *tile), bf),
            pltpu.VMEM((chunks, 2, 2, *tile), bf),
            dma((SLOTS, GROUPS + 1)),
            dma((SLOTS, GROUPS + 1)),
            dma((SLOTS, GROUPS + 1)),
            dma((2, 3)),
            dma((2, 2, 2)),
            dma((2, 2)),
            dma((chunks, 2)),
            dma((2, 2)),
            dma((chunks, 2)),
            dma((2, 2)),
            dma((len(parts),)),
            dma((2,)),
            dma((2,)),
            pltpu.SemaphoreType.REGULAR,
        ],
        compiler_params=pltpu.CompilerParams(collective_id=0, has_side_effects=True, vmem_limit_bytes=67_000_000),
        name="reduce",
    )(*terms, *weights, *ms, *vs)
    count = len(parts)
    return out[:count], out[count : 2 * count], list(out[2 * count : 2 * count + 3]), out[-2:]


def place_kernel(chips, jobs, *refs):
    out, buf, in_sem, out_sem = refs[-4:]
    me = lax.axis_index("dp")
    x, k = me // CORES, lax.rem(me, CORES)
    copies = []
    for i, (layer, layers, rows, step, at, block_rows, other) in enumerate(jobs):
        core = 1 - k if other else k
        block = lax.rem(x + step * (1 - 2 * core) + chips, chips) * CORES + core
        slot = buf.at[i, pl.ds(0, layers), pl.ds(0, rows)]
        into = out.at[pl.ds(layer, layers), pl.ds(pl.multiple_of(block * block_rows + at, 8), rows)]
        copies.append((pltpu.make_async_copy(refs[i], slot, in_sem.at[i]), pltpu.make_async_copy(slot, into, out_sem.at[i])))
        copies[i][0].start()
    for first, second in copies:
        first.wait()
        second.start()
    for _, second in copies:
        second.wait()


def place(chips, shape, pieces, so_far):
    arrays = [p[0] for p in pieces]
    jobs = [(p[1], *p[0].shape[:2], *p[2:]) for p in pieces]
    size = max(a.shape[0] for a in arrays), max(a.shape[1] for a in arrays), arrays[0].shape[2]
    extra = () if so_far is None else (so_far,)
    return pl.pallas_call(
        functools.partial(place_kernel, chips, jobs),
        out_shape=jax.ShapeDtypeStruct(shape, jnp.bfloat16),
        in_specs=[pl.BlockSpec(memory_space=pl.ANY)] * (len(jobs) + len(extra)),
        out_specs=pl.BlockSpec(memory_space=pl.ANY),
        scratch_shapes=[
            pltpu.VMEM((len(jobs), *size), jnp.bfloat16),
            pltpu.SemaphoreType.DMA((len(jobs),)),
            pltpu.SemaphoreType.DMA((len(jobs),)),
        ],
        input_output_aliases={len(jobs): 0} if extra else {},
        compiler_params=pltpu.CompilerParams(vmem_limit_bytes=67_000_000),
        cost_estimate=pl.CostEstimate(flops=20_000_000, bytes_accessed=4 * sum(a.size for a in arrays), transcendentals=0),
        name="place",
    )(*arrays, *extra)


def solution(mesh):
    n = mesh.shape["dp"]
    chips = n // CORES

    def pairs(step, flip=0):
        return [(x * CORES + k, (x + step * (1 - 2 * k)) % chips * CORES + (k + flip) % CORES) for x in range(chips) for k in range(CORES)]

    one_way, other_way, partner = pairs(1), pairs(-1), pairs(0, 1)

    def send(a, where):
        return lax.ppermute(a, "dp", where)

    def step(*arrays):
        terms, weights, ms, vs = (arrays[i : i + 3] for i in (0, 3, 6, 9))
        layers = terms[0].shape[1]
        f32 = jnp.float32
        parts = [(i, 0, layers) for i in range(2)] + [(2, layer, 1) for layer in range(layers)]
        fresh, other, gradients, first = reduce_and_step(chips, parts, terms, weights, ms, vs)

        last = len(parts) - 1
        whole, new_m, new_v = [None] * 3, [None] * 3, [None] * 3
        near, far, cuts = {0: first}, {}, {}
        for at, (i, start, size) in enumerate(parts):
            if at:
                near[at] = send(fresh[at], one_way), send(fresh[at], other_way)
            a, b = near[at]
            by_layer = size % 2 == 0
            half = (size if by_layer else a.shape[1]) // 2
            c, d = (a[:half], b[half:]) if by_layer else (a[:, :half], b[:, half:])
            cuts[at] = (start, 0), (start + half, 0) if by_layer else (start, half)
            far[at] = send(c, one_way), send(d, other_way)

        def put(at, pieces, apart=False):
            i = parts[at][0]
            rows = fresh[at].shape[1]
            theirs = [send(a, partner) if p is None else p for a, p, *_ in pieces]
            mine = [(p[0], *p[2:], rows, False) for p in pieces]
            theirs = [(t, *p[2:], rows, True) for t, p in zip(theirs, pieces)]
            if apart:
                whole[i] = place(chips, weights[i].shape, mine, whole[i])
                mine = []
            whole[i] = place(chips, weights[i].shape, mine + theirs, whole[i])

        for w in range(1, 3):
            c, d = far[w - 1]
            gradients[w], c = lax.optimization_barrier((gradients[w], c))
            far[w - 1] = c, d

        def put_far(at, apart=False):
            (c, d), ((c_layer, c_row), (d_layer, d_row)) = far[at], cuts[at]
            put(at, [(c, None, c_layer, 2, c_row), (d, None, d_layer, 2, d_row)], apart)

        for at in EARLY:
            put(at, [(fresh[at], other[at], parts[at][1], 0, 0)])
        for at, (i, start, _) in enumerate(parts):
            a, b = near[at]
            home = [] if at in EARLY else [(fresh[at], other[at], start, 0, 0)]
            put(at, home + [(a, None, start, chips - 1, 0), (b, None, start, 1, 0)], at == last)
            if at:
                put_far(at - 1, at == last)
        put_far(last, True)
        for w in range(3):
            g = gradients[w].astype(f32)
            new_m[w] = 0.9 * ms[w] + 0.1 * g
            new_v[w] = 0.95 * vs[w] + 0.05 * g * g
        return (*whole, *new_m, *new_v)

    all_of, cut = P(None, None, None), P(None, "dp", None)
    return jax.shard_map(
        step,
        mesh=mesh,
        in_specs=(P(("rep", "dp"), None, None, None),) * 3 + (all_of,) * 3 + (cut,) * 6,
        out_specs=(P("rep", None, None),) * 3 + (P("rep", "dp", None),) * 6,
        check_vma=False,
    )
```
